32 devices in a mesh: gx: 4 (over x, core), gy: 8 (over z, y).
Axes of the slice: x: 2, y: 2, z: 4, core: 2. Of those that a mesh axis runs over, the one named last changes fastest.
Arguments:
- log_crit: float32 [512, 512, 128], P('gx', 'gy'), may hold values from -4 to 4
- col_bins: int32 [512, 512, 4], P('gx', 'gy'), may hold values from 0 to 127
- rate_table: bfloat16 [128, 64], replicated, may hold values from 0.0039978027 to 0.059814453
- tile_mask: int32 [16, 16, 4], P('gx', 'gy'), may hold values from 0 to 1, as said below
- tile_route: int32 [16, 16, 4], P('gx', 'gy'), may hold values from 0 to 7, as said below
- filt_x: float32 [512], replicated, may hold values from 0.1 to 1, as said below
- filt_y: float32 [512], replicated, may hold values from 0.1 to 1, as said below
Outputs:
- recomb: float32 [512, 512, 128], P('gx', 'gy')
- smoothed: float32 [512, 512, 128], P('gx', 'gy')
- load: float32 [4, 8], P('gx', 'gy')
The draws below stay inside these ranges and needn't reach their ends.
Inputs may be any that keep to these rules, and one draw needn't show every extreme that they name: `tile_mask`: tiles form blocks of 4 x 2 x 4 (indices a // 4, b // 2); among the blocks with the same a // 4, some block has all 32 tiles active. `tile_route`: counting only tiles with tile_mask 1: among the blocks with the same a // 4 at most 16 active tiles share a route, and in every draw some such row of blocks gives every route exactly 16; at most 4 active tiles of one block share a route, and in every draw some block has 4 that do. filt_x[m] == filt_x[512 - m] for 0 < m < 512. filt_y[n] == filt_y[512 - n] for 0 < n < 512.
All inputs are finite; a program needn't handle non-finite values.
Results may differ from the reference program's by a relative error of at most 0.0003.
Values sent between devices are 32-bit elements; how exact they have to be, the bound alone decides.
No kernel may reach another device: no remote copies, remote signals or barrier semaphores. Data moves between devices by JAX's collectives and lax.ppermute only.
A program may use at most 128 MiB of HBM per device.

```python
import math
import jax
import jax.numpy as jnp
from jax import lax

TE = 32
TX = 4
TY = 2
TZ = 4
BINS = 128
NODES = 64
RECV = 16
NX = 512
NY = 512
NZ = 128
N_GX = 4
N_GY = 8


def tile_plan(key):
    base_key = jax.random.fold_in(key, 11)
    k_count, k_busy, k_row, k_perm, k_spare = jax.random.split(base_key, 5)
    tiles_block = TX * TY * TZ
    half_tiles = tiles_block // 2
    quarter_tiles = tiles_block // 4
    pair_cap = tiles_block // N_GY
    counts = jax.random.randint(k_count, (N_GX, N_GY), quarter_tiles, half_tiles)
    busiest = jax.random.randint(k_busy, (N_GX,), 0, N_GY)
    full_row = jax.random.randint(k_row, (), 0, N_GX)
    column_ids = jnp.arange(N_GY)[None, :]
    counts = jnp.where(jnp.arange(N_GX)[:, None] == full_row, half_tiles, counts)
    counts = jnp.where(column_ids == busiest[:, None], tiles_block, counts)
    counts = jnp.where(column_ids == (busiest[:, None] + 1) % N_GY, 0, counts)
    perm_keys = jax.random.split(k_perm, N_GX * N_GY)
    tile_ranks = jax.vmap(lambda sub_key: jax.random.permutation(sub_key, tiles_block))(perm_keys).reshape(N_GX, N_GY, tiles_block)
    active = (tile_ranks < counts[:, :, None]).astype(jnp.int32)
    row_flags = active.reshape(N_GX, N_GY * tiles_block)
    before = jnp.cumsum(row_flags, axis=1) - row_flags
    chosen = (before // pair_cap % N_GY).reshape(N_GX, N_GY, tiles_block)
    spare_route = jax.random.randint(k_spare, (N_GX, N_GY, tiles_block), 0, N_GY)
    routes = jnp.where(active == 1, chosen, spare_route).astype(jnp.int32)
    return (lay_out(active), lay_out(routes))


def lay_out(values):
    shaped = values.reshape(N_GX, N_GY, TX, TY, TZ).transpose(0, 2, 1, 3, 4)
    return shaped.reshape(N_GX * TX, N_GY * TY, TZ)


def window_draw(key, length):
    half = length // 2 + 1
    values = jnp.exp(jax.random.uniform(key, (half,), jnp.float32, math.log(0.1), 0.0))
    indices = jnp.arange(length)
    folded = jnp.minimum(indices, length - indices)
    return values[folded].astype(jnp.float32)


def draw_tile_mask(key, part):
    return tile_plan(key)[0]


def draw_tile_route(key, part):
    return tile_plan(key)[1]


def draw_filt_x(key, part):
    return window_draw(jax.random.fold_in(key, 21), NX)


def draw_filt_y(key, part):
    return window_draw(jax.random.fold_in(key, 23), NY)


def plant(result, own_key, smallest, largest):
    place = [jax.random.randint(jax.random.fold_in(own_key, axis), (), 0, length) for axis, length in enumerate(result.shape)]
    widest = result.shape.index(max(result.shape))
    beside = place[:widest] + [(place[widest] + 1) % result.shape[widest]] + place[widest + 1:]
    return result.at[tuple(place)].set(smallest).at[tuple(beside)].set(largest)


def block_scale(stream_key, dims, shards, low, largest):
    loudness = 1.0
    for position, parts in shards:
        heights = jax.random.uniform(jax.random.fold_in(jax.random.fold_in(stream_key, 6), position), (parts,), jnp.float32, low / len(shards), largest / len(shards))
        loudness = loudness * jnp.repeat(jnp.exp(heights), dims[position] // parts).reshape((-1,) + (1,) * (len(dims) - 1 - position))
    return loudness


def normal_values(own_key, shape, scale, reach, cuts=(), kind=jnp.bfloat16):
    drawn = scale * jax.random.normal(own_key, shape, jnp.float32)
    if cuts:
        drawn = drawn * block_scale(own_key, shape, cuts, -0.22, 0.18)
    return jnp.clip(drawn, -reach, reach).astype(kind)


def setup_inputs(seed: int = 0) -> dict:
    key_of = jax.random.split(jax.random.key(seed), 8)
    return {
        "log_crit": normal_values(key_of[0], (NX, NY, NZ), 1.0, 4.0, ((0, 4), (1, 8)), jnp.float32),
        "col_bins": plant(jax.random.randint(key_of[1], (NX, NY, TZ), 0, BINS), jax.random.fold_in(key_of[1], 1), 0, BINS - 1).astype(jnp.int32),
        "rate_table": jnp.clip(jnp.exp(jax.random.uniform(key_of[2], (BINS, NODES), jnp.float32, math.log(0.0039978027), math.log(0.059814453))), 0.0039978027, 0.059814453).astype(jnp.bfloat16),
        "tile_mask": draw_tile_mask(jax.random.fold_in(key_of[7], 71), 0),
        "tile_route": draw_tile_route(jax.random.fold_in(key_of[7], 71), 0),
        "filt_x": draw_filt_x(jax.random.fold_in(key_of[7], 71), 0),
        "filt_y": draw_filt_y(jax.random.fold_in(key_of[7], 71), 0),
    }


steepness = 3.0


def reference(log_crit, col_bins, rate_table, tile_mask, tile_route, filt_x, filt_y):
    size_x, size_y, size_z = log_crit.shape
    rows_x = N_GX * TX
    rows_y = N_GY * TY
    tile_cells = log_crit.reshape(rows_x, TE, rows_y, TE, TZ, TE).transpose(0, 2, 4, 1, 3, 5).reshape(-1, TE, TE, TE)
    tile_bins = col_bins.reshape(rows_x, TE, rows_y, TE, TZ).transpose(0, 2, 4, 1, 3).reshape(-1, TE, TE)
    live_flags = tile_mask.reshape(-1)
    table_f32 = rate_table.astype(jnp.float32)
    node_grid = -2.5 + 5.0 * jnp.arange(NODES, dtype=jnp.float32) / (NODES - 1)

    def tile_value(operands):
        field, bin_cols, is_live = operands
        table_rows = table_f32[bin_cols]

        def active(unused):
            cutoff = jax.nn.sigmoid((field[..., None] - node_grid) * steepness)
            return jnp.sum(cutoff * table_rows[:, :, None, :], axis=-1)

        def quiet(unused):
            return jnp.zeros_like(field)

        return lax.cond(is_live == 1, active, quiet, 0)

    values = lax.map(tile_value, (tile_cells, tile_bins, live_flags))
    tile_mean = jnp.mean(values.reshape(values.shape[0], -1), axis=1).reshape(rows_x, rows_y, TZ)
    onehot = (tile_route[..., None] == jnp.arange(N_GY)).astype(jnp.float32)
    per_row = jnp.einsum('abt,abtg->ag', tile_mean.astype(jnp.float32), onehot)
    load = jnp.sum(per_row.reshape(N_GX, TX, N_GY), axis=1) / RECV
    recomb = values.reshape(rows_x, rows_y, TZ, TE, TE, TE).transpose(0, 3, 1, 4, 2, 5).reshape(size_x, size_y, size_z)
    gain_plane = filt_x[:, None, None] * filt_y[None, :, None]
    z_block = 16 if size_z % 16 == 0 else size_z
    blocks = recomb.reshape(size_x, size_y, size_z // z_block, z_block).transpose(2, 0, 1, 3)

    def smooth_block(block):
        spectrum = jnp.fft.fft2(block, axes=(0, 1))
        return jnp.real(jnp.fft.ifft2(spectrum * gain_plane, axes=(0, 1))).astype(jnp.float32)

    smoothed = lax.map(smooth_block, blocks).transpose(1, 2, 0, 3).reshape(size_x, size_y, size_z)
    return recomb, smoothed, load
```

```python
import functools

import jax
import jax.numpy as jnp
import numpy as np
from jax import lax
from jax.experimental import pallas as pl
from jax.experimental.pallas import tpu as pltpu
from jax.sharding import PartitionSpec as P

STEEPNESS = 3.0
ROWS = 8
VMEM_BYTES = 40 * 1024 * 1024


def node_grid(nodes):
    return np.float32(-2.5) + np.float32(5.0) * np.arange(nodes, dtype=np.float32) / np.float32(nodes - 1)


def evaluate_kernel(run_first, runs, edge, devices, mask_ref, field_ref, bins_ref, rate_ref, cells_ref, sums_ref, row_scratch, field_scratch):
    step = pl.program_id(0)
    size_x, rows, size_z = field_ref.shape
    nodes, levels = rate_ref.shape
    planes = cells_ref.shape[1]
    half_nodes = np.float32(0.5 * STEEPNESS) * node_grid(nodes)
    tile_b = step * rows // edge
    tiles_x = size_x // edge
    lane = lax.broadcasted_iota(jnp.int32, (1, size_x), 1)
    level = lax.broadcasted_iota(jnp.int32, (levels, size_x), 0)
    field = field_ref.reshape(size_x * rows, size_z)
    cells = cells_ref.reshape(devices * planes * rows, size_x)

    @pl.when(step % (edge // rows) == 0)
    def _():
        sums_ref[...] = jnp.zeros_like(sums_ref)

    for run in range(runs):
        active = jnp.zeros((1, size_x), jnp.float32)
        for a in range(tiles_x):
            flag = mask_ref[a, tile_b, run_first + run]
            here = (lane >= a * edge) & (lane < (a + 1) * edge)
            active = jnp.where(here & (flag == 1), 0.5, active)
        for y in range(rows):
            onehot = (level == bins_ref[y, pl.ds(run_first + run, 1), :]).astype(jnp.bfloat16)
            row_scratch[run, y] = jnp.dot(rate_ref[...], onehot, preferred_element_type=jnp.float32) * active

    def one_row(y, carry):
        turned = field[pl.ds(y, size_x, stride=rows), :].T
        scaled = (turned * (0.5 * STEEPNESS))[run_first * edge : (run_first + runs) * edge]
        for run in range(runs):
            values = scaled[run * edge : (run + 1) * edge]
            total = jnp.broadcast_to(jnp.sum(row_scratch[run, y], axis=0, keepdims=True), values.shape)
            for q in range(nodes):
                rate = row_scratch[run, y, pl.ds(q, 1), :]
                total = total + rate * jnp.tanh(values - half_nodes[q])
            plane, first = divmod(run * edge, devices)
            cells[pl.ds(first * planes * rows + plane * rows + y, edge, stride=planes * rows), :] = total
            part = total[0:8]
            for k in range(8, edge, 8):
                part = part + total[k : k + 8]
            sums_ref[0, run] += part
        return carry

    lax.fori_loop(0, rows, one_row, 0)


def evaluate(log_crit, bins, rates, tile_mask, run_first, runs, devices):
    size_x, size_y, size_z = log_crit.shape
    edge = size_x // tile_mask.shape[0]
    planes = runs * edge // devices
    tiles_y = tile_mask.shape[1]
    nodes, levels = rates.shape
    steps = size_y // ROWS
    return pl.pallas_call(
        functools.partial(evaluate_kernel, run_first, runs, edge, devices),
        grid=(steps,),
        in_specs=[
            pl.BlockSpec(memory_space=pltpu.SMEM),
            pl.BlockSpec((size_x, ROWS, size_z), lambda j: (0, j, 0)),
            pl.BlockSpec((ROWS, bins.shape[1], size_x), lambda j: (j, 0, 0)),
            pl.BlockSpec((nodes, levels), lambda j: (0, 0)),
        ],
        out_specs=[
            pl.BlockSpec((devices, planes, ROWS, size_x), lambda j: (0, 0, j, 0)),
            pl.BlockSpec((1, runs, 8, size_x), lambda j: (j * ROWS // edge, 0, 0, 0)),
        ],
        out_shape=[
            jax.ShapeDtypeStruct((devices, planes, size_y, size_x), jnp.float32),
            jax.ShapeDtypeStruct((tiles_y, runs, 8, size_x), jnp.float32),
        ],
        scratch_shapes=[
            pltpu.VMEM((runs, ROWS, nodes, size_x), jnp.float32),
            pltpu.VMEM((size_z, size_x), jnp.float32),
        ],
        cost_estimate=pl.CostEstimate(
            flops=runs * edge * size_x * size_y * nodes * 4, bytes_accessed=6 << 20, transcendentals=0
        ),
        compiler_params=pltpu.CompilerParams(vmem_limit_bytes=VMEM_BYTES),
        name="evaluate",
    )(tile_mask, log_crit, bins, rates)


def split(value):
    high = value.astype(jnp.bfloat16)
    low = (value - high.astype(jnp.float32)).astype(jnp.bfloat16)
    return high, low


def product(left, right):
    dot = functools.partial(jnp.dot, preferred_element_type=jnp.float32)
    return dot(left[0], right[0]) + (dot(left[0], right[1]) + dot(left[1], right[0]))


def window_kernel(span_x, span_y, x_ref, y_ref, plane_ref, out_ref):
    rows, lanes = plane_ref.shape[-2:]
    plane = jnp.concatenate(
        [
            jnp.concatenate([plane_ref[i * span_y + j, 0] for i in range(span_x)], axis=1)
            for j in range(span_y)
        ],
        axis=0,
    )
    along_y = product(split(y_ref[...]), split(plane))
    both = product(split(along_y), split(x_ref[...]))
    for i in range(span_x):
        for j in range(span_y):
            out_ref[i * span_y + j, 0] = both[j * rows : (j + 1) * rows, i * lanes : (i + 1) * lanes]


def apply_window(planes, matrix_x, matrix_y, span_x, span_y):
    devices, count, rows, lanes = planes.shape
    size_x, size_y = matrix_x.shape[0], matrix_y.shape[0]
    spec = pl.BlockSpec((devices, 1, rows, lanes), lambda p: (0, p, 0, 0))
    return pl.pallas_call(
        functools.partial(window_kernel, span_x, span_y),
        grid=(count,),
        in_specs=[
            pl.BlockSpec((size_x, size_x), lambda p: (0, 0)),
            pl.BlockSpec((size_y, size_y), lambda p: (0, 0)),
            spec,
        ],
        out_specs=spec,
        out_shape=jax.ShapeDtypeStruct(planes.shape, jnp.float32),
        cost_estimate=pl.CostEstimate(
            flops=count * 6 * size_x * size_y * (size_x + size_y), bytes_accessed=4 << 20, transcendentals=0
        ),
        compiler_params=pltpu.CompilerParams(vmem_limit_bytes=VMEM_BYTES),
        name="window",
    )(matrix_x, matrix_y, planes)


def restore_kernel(edge, count, *refs):
    parts, out_ref = refs[:count], refs[count]
    size_x, rows, size_z = out_ref.shape
    out = out_ref.reshape(size_x * rows, size_z)

    def one_row(y, carry):
        pieces = []
        for part in parts:
            devices, planes = part.shape[:2]
            flat = part.reshape(devices * planes * rows, size_x)
            for plane in range(planes):
                pieces.append(flat[pl.ds(plane * rows + y, devices, stride=planes * rows), :])
        whole = pieces[0] if len(pieces) == 1 else jnp.concatenate(pieces, axis=0)
        out[pl.ds(y, size_x, stride=rows), :] = whole.T
        return carry

    lax.fori_loop(0, rows, one_row, 0)


def restore(parts, edge):
    size_y, size_x = parts[0].shape[2:]
    size_z = sum(part.shape[0] * part.shape[1] for part in parts)
    return pl.pallas_call(
        functools.partial(restore_kernel, edge, len(parts)),
        grid=(size_y // ROWS,),
        in_specs=[
            pl.BlockSpec((*part.shape[:2], ROWS, size_x), lambda j: (0, 0, j, 0)) for part in parts
        ],
        out_specs=pl.BlockSpec((size_x, ROWS, size_z), lambda j: (0, j, 0)),
        out_shape=jax.ShapeDtypeStruct((size_x, size_y, size_z), jnp.float32),
        cost_estimate=pl.CostEstimate(flops=1 << 30, bytes_accessed=8 << 20, transcendentals=0),
        compiler_params=pltpu.CompilerParams(vmem_limit_bytes=VMEM_BYTES),
        name="restore",
    )(*parts)


def wave_table(length):
    half = length // 2
    freq = np.concatenate([np.arange(half + 1), np.arange(1, half)])
    angle = 2.0 * np.pi / length * (np.arange(length)[:, None] * freq[None, :] % length)
    table = np.where(np.arange(length)[None, :] <= half, np.cos(angle), np.sin(angle))
    doubled = np.where((freq == 0) | (freq == half), 1.0, 2.0) / length
    return table.astype(np.float32), doubled.astype(np.float32)


def window_matrix(gain, table, doubled):
    length = gain.shape[0]
    half = length // 2
    weight = jnp.concatenate([gain[: half + 1], gain[1:half]]) * doubled
    return lax.dot_general(
        table * weight[None, :], table, (((1,), (1,)), ((), ())), precision=lax.Precision.HIGHEST
    )


def on_device(groups, log_crit, col_bins, rate_table, tile_mask, tile_route, filt_x, filt_y):
    span_x, span_y = lax.axis_size("gx"), lax.axis_size("gy")
    devices = span_x * span_y
    size_x, size_y, size_z = log_crit.shape
    blocks_x, blocks_y, blocks_z = tile_mask.shape
    edge = size_x // blocks_x
    tile_count = blocks_x * blocks_y * blocks_z
    bins = col_bins.transpose(1, 2, 0)
    rates = rate_table.T
    cells, sums = [], []
    for first, runs in groups:
        part, total = evaluate(log_crit, bins, rates, tile_mask, first, runs, devices)
        cells.append(part)
        sums.append(total)
    tables = {length: wave_table(length) for length in (filt_x.shape[0], filt_y.shape[0])}
    tables = {length: tuple(jnp.asarray(item) for item in pair) for length, pair in tables.items()}
    matrix_x = window_matrix(filt_x, *tables[filt_x.shape[0]])
    matrix_y = window_matrix(filt_y, *tables[filt_y.shape[0]])
    exchange = functools.partial(
        lax.all_to_all, axis_name=("gx", "gy"), split_axis=0, concat_axis=0, tiled=True
    )
    pencils = [exchange(part) for part in cells]
    filtered = [apply_window(part, matrix_x, matrix_y, span_x, span_y) for part in pencils]
    returned = [exchange(part) for part in filtered]
    recomb = restore(cells, edge)
    smoothed = restore(returned, edge)
    tile_sums = jnp.concatenate(sums, axis=1).sum(axis=2)
    tile_means = tile_sums.reshape(blocks_y, blocks_z, blocks_x, edge).sum(axis=3) / (edge * edge * edge)
    route = tile_route.transpose(1, 2, 0)
    workers = jnp.arange(span_y, dtype=jnp.int32)
    shares = jnp.where(route[..., None] == workers, tile_means[..., None], 0.0)
    contribution = shares.sum(axis=(0, 1, 2)) / (tile_count // 2)
    load = lax.psum_scatter(contribution, "gy", scatter_dimension=0, tiled=True)
    return recomb, smoothed, load.reshape(1, 1)


def split_runs(size_z, edge, devices):
    runs = size_z // edge
    smallest = max(1, devices // edge)
    if smallest * 2 > runs:
        return ((0, runs),)
    half = runs // 2
    return ((0, half), (half, runs - half))


def solution(mesh):
    placed = (
        P("gx", "gy", None),
        P("gx", "gy", None),
        P(),
        P("gx", "gy", None),
        P("gx", "gy", None),
        P(),
        P(),
    )
    devices = mesh.shape["gx"] * mesh.shape["gy"]

    def whole(*args):
        size_z = args[0].shape[2]
        edge = args[0].shape[0] // args[3].shape[0]
        groups = split_runs(size_z, edge, devices)
        return jax.shard_map(
            functools.partial(on_device, groups),
            mesh=mesh,
            in_specs=placed,
            out_specs=(P("gx", "gy", None), P("gx", "gy", None), P("gx", "gy")),
            check_vma=False,
        )(*args)

    return whole
```

```python
import functools

import jax
import jax.numpy as jnp
import numpy as np
from jax import lax
from jax.experimental import pallas as pl
from jax.experimental.pallas import tpu as pltpu
from jax.sharding import PartitionSpec as P

STEEPNESS = 3.0
ROWS = 16
UNROLL = 4


def node_grid(nodes):
    return np.float32(-2.5) + np.float32(5.0) * np.arange(nodes, dtype=np.float32) / np.float32(nodes - 1)


def evaluate_kernel(run_first, runs, edge, devices, mask_ref, field_ref, bins_ref, rate_ref, cells_ref, sums_ref, row_scratch):
    step = pl.program_id(0)
    size_x, rows, size_z = field_ref.shape
    nodes, levels = rate_ref.shape
    planes = cells_ref.shape[1]
    half_nodes = np.float32(0.5 * STEEPNESS) * node_grid(nodes)
    tile_b = step * rows // edge
    tiles_x = size_x // edge
    lane = lax.broadcasted_iota(jnp.int32, (1, size_x), 1)
    level = lax.broadcasted_iota(jnp.int32, (levels, size_x), 0)
    field = field_ref.reshape(size_x * rows, size_z)
    cells = cells_ref.reshape(devices * planes * rows, size_x)

    @pl.when(step % (edge // rows) == 0)
    def _():
        sums_ref[...] = jnp.zeros_like(sums_ref)

    for run in range(runs):
        active = jnp.zeros((1, size_x), jnp.float32)
        for a in range(tiles_x):
            flag = mask_ref[a, tile_b, run_first + run]
            here = (lane >= a * edge) & (lane < (a + 1) * edge)
            active = jnp.where(here & (flag == 1), 0.5, active)
        for y in range(rows):
            onehot = (level == bins_ref[y, pl.ds(run_first + run, 1), :]).astype(jnp.bfloat16)
            row_scratch[run, y] = jnp.dot(rate_ref[...], onehot, preferred_element_type=jnp.float32) * active

    first_z = run_first * edge
    last_z = first_z + runs * edge

    def some_rows(pair, carry):
        for y in [pair * UNROLL + k for k in range(UNROLL)]:
            if first_z == 0:
                turned = field[pl.ds(y, size_x, stride=rows), :][:, :last_z].T
            else:
                turned = field[pl.ds(y, size_x, stride=rows), :].T[first_z:last_z]
            scaled = turned * (0.5 * STEEPNESS)
            for run in range(runs):
                values = scaled[run * edge : (run + 1) * edge]
                total = jnp.broadcast_to(jnp.sum(row_scratch[run, y], axis=0, keepdims=True), values.shape)
                for q in range(nodes):
                    rate = row_scratch[run, y, pl.ds(q, 1), :]
                    total = total + rate * jnp.tanh(values - half_nodes[q])
                plane, first = divmod(run * edge, devices)
                cells[pl.ds(first * planes * rows + plane * rows + y, edge, stride=planes * rows), :] = total
                part = total[0:8]
                for k in range(8, edge, 8):
                    part = part + total[k : k + 8]
                sums_ref[0, run] += part
        return carry

    lax.fori_loop(0, rows // UNROLL, some_rows, 0)


def evaluate(log_crit, bins, rates, tile_mask, run_first, runs, devices):
    size_x, size_y, size_z = log_crit.shape
    edge = size_x // tile_mask.shape[0]
    planes = runs * edge // devices
    tiles_y = tile_mask.shape[1]
    nodes, levels = rates.shape
    steps = size_y // ROWS
    return pl.pallas_call(
        functools.partial(evaluate_kernel, run_first, runs, edge, devices),
        grid=(steps,),
        in_specs=[
            pl.BlockSpec(memory_space=pltpu.SMEM),
            pl.BlockSpec((size_x, ROWS, size_z), lambda j: (0, j, 0)),
            pl.BlockSpec((ROWS, bins.shape[1], size_x), lambda j: (j, 0, 0)),
            pl.BlockSpec((nodes, levels), lambda j: (0, 0)),
        ],
        out_specs=[
            pl.BlockSpec((devices, planes, ROWS, size_x), lambda j: (0, 0, j, 0)),
            pl.BlockSpec((1, runs, 8, size_x), lambda j: (j * ROWS // edge, 0, 0, 0)),
        ],
        out_shape=[
            jax.ShapeDtypeStruct((devices, planes, size_y, size_x), jnp.float32),
            jax.ShapeDtypeStruct((tiles_y, runs, 8, size_x), jnp.float32),
        ],
        scratch_shapes=[
            pltpu.VMEM((runs, ROWS, nodes, size_x), jnp.float32),
        ],
        cost_estimate=pl.CostEstimate(
            flops=runs * edge * size_x * size_y * nodes * 4, bytes_accessed=6 << 20, transcendentals=0
        ),
        name="evaluate",
    )(tile_mask, log_crit, bins, rates)


def split(value):
    high = value.astype(jnp.bfloat16)
    low = (value - high.astype(jnp.float32)).astype(jnp.bfloat16)
    return high, low


def product(left, right):
    dot = functools.partial(jnp.dot, preferred_element_type=jnp.float32)
    return dot(left[0], right[0]) + (dot(left[0], right[1]) + dot(left[1], right[0]))


def window_kernel(span_x, span_y, x_ref, y_ref, plane_ref, out_ref):
    rows, lanes = plane_ref.shape[-2:]
    plane = jnp.concatenate(
        [
            jnp.concatenate([plane_ref[i * span_y + j, 0] for i in range(span_x)], axis=1)
            for j in range(span_y)
        ],
        axis=0,
    )
    along_y = product(split(y_ref[...]), split(plane))
    both = product(split(along_y), split(x_ref[...]))
    for i in range(span_x):
        for j in range(span_y):
            out_ref[i * span_y + j, 0] = both[j * rows : (j + 1) * rows, i * lanes : (i + 1) * lanes]


def apply_window(planes, matrix_x, matrix_y, span_x, span_y):
    devices, count, rows, lanes = planes.shape
    size_x, size_y = matrix_x.shape[0], matrix_y.shape[0]
    spec = pl.BlockSpec((devices, 1, rows, lanes), lambda p: (0, p, 0, 0))
    return pl.pallas_call(
        functools.partial(window_kernel, span_x, span_y),
        grid=(count,),
        in_specs=[
            pl.BlockSpec((size_x, size_x), lambda p: (0, 0)),
            pl.BlockSpec((size_y, size_y), lambda p: (0, 0)),
            spec,
        ],
        out_specs=spec,
        out_shape=jax.ShapeDtypeStruct(planes.shape, jnp.float32),
        cost_estimate=pl.CostEstimate(
            flops=count * 6 * size_x * size_y * (size_x + size_y), bytes_accessed=4 << 20, transcendentals=0
        ),
        name="window",
    )(matrix_x, matrix_y, planes)


def restore_kernel(edge, count, *refs):
    parts, out_ref = refs[:count], refs[count]
    size_x, rows, size_z = out_ref.shape
    out = out_ref.reshape(size_x * rows, size_z)

    for y in range(rows):
        pieces = []
        for part in parts:
            devices, planes = part.shape[:2]
            flat = part.reshape(devices * planes * rows, size_x)
            for plane in range(planes):
                pieces.append(flat[pl.ds(plane * rows + y, devices, stride=planes * rows), :])
        whole = pieces[0] if len(pieces) == 1 else jnp.concatenate(pieces, axis=0)
        out[pl.ds(y, size_x, stride=rows), :] = whole.T


def restore(parts, edge):
    size_y, size_x = parts[0].shape[2:]
    size_z = sum(part.shape[0] * part.shape[1] for part in parts)
    return pl.pallas_call(
        functools.partial(restore_kernel, edge, len(parts)),
        grid=(size_y // ROWS,),
        in_specs=[
            pl.BlockSpec((*part.shape[:2], ROWS, size_x), lambda j: (0, 0, j, 0)) for part in parts
        ],
        out_specs=pl.BlockSpec((size_x, ROWS, size_z), lambda j: (0, j, 0)),
        out_shape=jax.ShapeDtypeStruct((size_x, size_y, size_z), jnp.float32),
        cost_estimate=pl.CostEstimate(flops=1 << 30, bytes_accessed=8 << 20, transcendentals=0),
        name="restore",
    )(*parts)


def wave_table(length):
    half = length // 2
    freq = np.concatenate([np.arange(half + 1), np.arange(1, half)])
    angle = 2.0 * np.pi / length * (np.arange(length)[:, None] * freq[None, :] % length)
    table = np.where(np.arange(length)[None, :] <= half, np.cos(angle), np.sin(angle))
    doubled = np.where((freq == 0) | (freq == half), 1.0, 2.0) / length
    return table.astype(np.float32), doubled.astype(np.float32)


def window_matrix(gain, table, doubled):
    length = gain.shape[0]
    half = length // 2
    weight = jnp.concatenate([gain[: half + 1], gain[1:half]]) * doubled
    return lax.dot_general(
        table * weight[None, :], table, (((1,), (1,)), ((), ())), precision=lax.Precision.HIGHEST
    )


def on_device(groups, log_crit, col_bins, rate_table, tile_mask, tile_route, filt_x, filt_y):
    span_x, span_y = lax.axis_size("gx"), lax.axis_size("gy")
    devices = span_x * span_y
    size_x, size_y, size_z = log_crit.shape
    blocks_x, blocks_y, blocks_z = tile_mask.shape
    edge = size_x // blocks_x
    tile_count = blocks_x * blocks_y * blocks_z
    bins = col_bins.transpose(1, 2, 0)
    rates = rate_table.T
    cells, sums = [], []
    for first, runs in groups:
        part, total = evaluate(log_crit, bins, rates, tile_mask, first, runs, devices)
        cells.append(part)
        sums.append(total)
    tables = {length: wave_table(length) for length in (filt_x.shape[0], filt_y.shape[0])}
    tables = {length: tuple(jnp.asarray(item) for item in pair) for length, pair in tables.items()}
    matrix_x = window_matrix(filt_x, *tables[filt_x.shape[0]])
    matrix_y = window_matrix(filt_y, *tables[filt_y.shape[0]])
    exchange = functools.partial(
        lax.all_to_all, axis_name=("gx", "gy"), split_axis=0, concat_axis=0, tiled=True
    )
    tile_sums = jnp.concatenate(sums, axis=1).sum(axis=2)
    tile_means = tile_sums.reshape(blocks_y, blocks_z, blocks_x, edge).sum(axis=3) / (edge * edge * edge)
    route = tile_route.transpose(1, 2, 0)
    workers = jnp.arange(span_y, dtype=jnp.int32)
    shares = jnp.where(route[..., None] == workers, tile_means[..., None], 0.0)
    contribution = shares.sum(axis=(0, 1, 2)) / (tile_count // 2)
    pencils = [exchange(part) for part in cells]
    recomb = restore(cells, edge)
    filtered = [apply_window(part, matrix_x, matrix_y, span_x, span_y) for part in pencils]
    filtered[0], recomb = lax.optimization_barrier((filtered[0], recomb))
    filtered[-1], contribution = lax.optimization_barrier((filtered[-1], contribution))
    returned = [exchange(part) for part in filtered]
    mine = workers == lax.axis_index("gy")
    load = jnp.sum(jnp.where(mine, lax.psum(contribution, "gy"), 0.0)).reshape(1, 1)
    smoothed = restore(returned, edge)
    return recomb, smoothed, load


def split_runs(size_z, edge, devices):
    runs = size_z // edge
    smallest = max(1, devices // edge)
    if smallest * 2 > runs:
        return ((0, runs),)
    return ((0, smallest), (smallest, runs - smallest))


def solution(mesh):
    placed = (
        P("gx", "gy", None),
        P("gx", "gy", None),
        P(),
        P("gx", "gy", None),
        P("gx", "gy", None),
        P(),
        P(),
    )
    devices = mesh.shape["gx"] * mesh.shape["gy"]

    def whole(*args):
        size_z = args[0].shape[2]
        edge = args[0].shape[0] // args[3].shape[0]
        groups = split_runs(size_z, edge, devices)
        return jax.shard_map(
            functools.partial(on_device, groups),
            mesh=mesh,
            in_specs=placed,
            out_specs=(P("gx", "gy", None), P("gx", "gy", None), P("gx", "gy")),
            check_vma=False,
        )(*args)

    return whole
```

```python
import functools

import jax
import jax.numpy as jnp
import numpy as np
from jax import lax
from jax.experimental import pallas as pl
from jax.experimental.pallas import tpu as pltpu
from jax.sharding import PartitionSpec as P

STEEPNESS = 3.0
ROWS = 16
UNROLL = 4


def node_grid(nodes):
    return np.float32(-2.5) + np.float32(5.0) * np.arange(nodes, dtype=np.float32) / np.float32(nodes - 1)


def evaluate_kernel(run_first, runs, edge, devices, mask_ref, field_ref, bins_ref, rate_ref, cells_ref, sums_ref, row_scratch):
    step = pl.program_id(0)
    size_x, rows, size_z = field_ref.shape
    nodes, levels = rate_ref.shape
    planes = cells_ref.shape[1]
    half_nodes = np.float32(0.5 * STEEPNESS) * node_grid(nodes)
    tile_b = step * rows // edge
    tiles_x = size_x // edge
    lane = lax.broadcasted_iota(jnp.int32, (1, size_x), 1)
    level = lax.broadcasted_iota(jnp.int32, (levels, size_x), 0)
    field = field_ref.reshape(size_x * rows, size_z)
    cells = cells_ref.reshape(devices * planes * rows, size_x)

    @pl.when(step % (edge // rows) == 0)
    def _():
        sums_ref[...] = jnp.zeros_like(sums_ref)

    for run in range(runs):
        active = jnp.zeros((1, size_x), jnp.float32)
        for a in range(tiles_x):
            flag = mask_ref[a, tile_b, run_first + run]
            here = (lane >= a * edge) & (lane < (a + 1) * edge)
            active = jnp.where(here & (flag == 1), 0.5, active)
        for y in range(rows):
            onehot = (level == bins_ref[y, pl.ds(run_first + run, 1), :]).astype(jnp.bfloat16)
            row_scratch[run, y] = jnp.dot(rate_ref[...], onehot, preferred_element_type=jnp.float32) * active

    first_z = run_first * edge
    last_z = first_z + runs * edge

    def some_rows(pair, carry):
        for y in [pair * UNROLL + k for k in range(UNROLL)]:
            if first_z == 0:
                turned = field[pl.ds(y, size_x, stride=rows), :][:, :last_z].T
            else:
                turned = field[pl.ds(y, size_x, stride=rows), :].T[first_z:last_z]
            scaled = turned * (0.5 * STEEPNESS)
            for run in range(runs):
                values = scaled[run * edge : (run + 1) * edge]
                total = jnp.broadcast_to(jnp.sum(row_scratch[run, y], axis=0, keepdims=True), values.shape)
                for q in range(nodes):
                    rate = row_scratch[run, y, pl.ds(q, 1), :]
                    total = total + rate * jnp.tanh(values - half_nodes[q])
                plane, first = divmod(run * edge, devices)
                cells[pl.ds(first * planes * rows + plane * rows + y, edge, stride=planes * rows), :] = total
                part = total[0:8]
                for k in range(8, edge, 8):
                    part = part + total[k : k + 8]
                sums_ref[0, run] += part
        return carry

    lax.fori_loop(0, rows // UNROLL, some_rows, 0)


def evaluate(log_crit, bins, rates, tile_mask, run_first, runs, devices):
    size_x, size_y, size_z = log_crit.shape
    edge = size_x // tile_mask.shape[0]
    planes = runs * edge // devices
    tiles_y = tile_mask.shape[1]
    nodes, levels = rates.shape
    steps = size_y // ROWS
    return pl.pallas_call(
        functools.partial(evaluate_kernel, run_first, runs, edge, devices),
        grid=(steps,),
        in_specs=[
            pl.BlockSpec(memory_space=pltpu.SMEM),
            pl.BlockSpec((size_x, ROWS, size_z), lambda j: (0, j, 0)),
            pl.BlockSpec((ROWS, bins.shape[1], size_x), lambda j: (j, 0, 0)),
            pl.BlockSpec((nodes, levels), lambda j: (0, 0)),
        ],
        out_specs=[
            pl.BlockSpec((devices, planes, ROWS, size_x), lambda j: (0, 0, j, 0)),
            pl.BlockSpec((1, runs, 8, size_x), lambda j: (j * ROWS // edge, 0, 0, 0)),
        ],
        out_shape=[
            jax.ShapeDtypeStruct((devices, planes, size_y, size_x), jnp.float32),
            jax.ShapeDtypeStruct((tiles_y, runs, 8, size_x), jnp.float32),
        ],
        scratch_shapes=[
            pltpu.VMEM((runs, ROWS, nodes, size_x), jnp.float32),
        ],
        cost_estimate=pl.CostEstimate(
            flops=runs * edge * size_x * size_y * nodes * 4, bytes_accessed=6 << 20, transcendentals=0
        ),
        name="evaluate",
    )(tile_mask, log_crit, bins, rates)


def split(value):
    high = value.astype(jnp.bfloat16)
    low = (value - high.astype(jnp.float32)).astype(jnp.bfloat16)
    return high, low


def product(left, right):
    dot = functools.partial(jnp.dot, preferred_element_type=jnp.float32)
    return dot(left[0], right[0]) + (dot(left[0], right[1]) + dot(left[1], right[0]))


def window_kernel(span_x, span_y, first_planes, x_ref, y_ref, *refs):
    plane_refs, out_ref = refs[:-1], refs[-1]
    rows, lanes = out_ref.shape[-2:]
    step = pl.program_id(0)

    def assemble(ref):
        return jnp.concatenate(
            [
                jnp.concatenate([ref[i * span_y + j, 0] for i in range(span_x)], axis=1)
                for j in range(span_y)
            ],
            axis=0,
        )

    plane = assemble(plane_refs[0])
    if len(plane_refs) == 2:
        plane = jnp.where(step < first_planes, plane, assemble(plane_refs[1]))
    along_y = product(split(y_ref[...]), split(plane))
    both = product(split(along_y), split(x_ref[...]))
    for i in range(span_x):
        for j in range(span_y):
            out_ref[i * span_y + j, 0] = both[j * rows : (j + 1) * rows, i * lanes : (i + 1) * lanes]


def apply_window(parts, matrix_x, matrix_y, span_x, span_y):
    devices, first_planes, rows, lanes = parts[0].shape
    count = sum(part.shape[1] for part in parts)
    size_x, size_y = matrix_x.shape[0], matrix_y.shape[0]
    block = (devices, 1, rows, lanes)
    specs = [pl.BlockSpec(block, lambda p: (0, jnp.minimum(p, first_planes - 1), 0, 0))]
    if len(parts) == 2:
        specs.append(pl.BlockSpec(block, lambda p: (0, jnp.maximum(p - first_planes, 0), 0, 0)))
    return pl.pallas_call(
        functools.partial(window_kernel, span_x, span_y, first_planes),
        grid=(count,),
        in_specs=[
            pl.BlockSpec((size_x, size_x), lambda p: (0, 0)),
            pl.BlockSpec((size_y, size_y), lambda p: (0, 0)),
            *specs,
        ],
        out_specs=pl.BlockSpec(block, lambda p: (0, p, 0, 0)),
        out_shape=jax.ShapeDtypeStruct((devices, count, rows, lanes), jnp.float32),
        cost_estimate=pl.CostEstimate(
            flops=count * 6 * size_x * size_y * (size_x + size_y), bytes_accessed=4 << 20, transcendentals=0
        ),
        name="window",
    )(matrix_x, matrix_y, *parts)


def restore_kernel(edge, count, *refs):
    parts, out_ref = refs[:count], refs[count]
    size_x, rows, size_z = out_ref.shape
    out = out_ref.reshape(size_x * rows, size_z)

    for y in range(rows):
        pieces = []
        for part in parts:
            devices, planes = part.shape[:2]
            flat = part.reshape(devices * planes * rows, size_x)
            for plane in range(planes):
                pieces.append(flat[pl.ds(plane * rows + y, devices, stride=planes * rows), :])
        whole = pieces[0] if len(pieces) == 1 else jnp.concatenate(pieces, axis=0)
        out[pl.ds(y, size_x, stride=rows), :] = whole.T


def restore(parts, edge):
    size_y, size_x = parts[0].shape[2:]
    size_z = sum(part.shape[0] * part.shape[1] for part in parts)
    return pl.pallas_call(
        functools.partial(restore_kernel, edge, len(parts)),
        grid=(size_y // ROWS,),
        in_specs=[
            pl.BlockSpec((*part.shape[:2], ROWS, size_x), lambda j: (0, 0, j, 0)) for part in parts
        ],
        out_specs=pl.BlockSpec((size_x, ROWS, size_z), lambda j: (0, j, 0)),
        out_shape=jax.ShapeDtypeStruct((size_x, size_y, size_z), jnp.float32),
        cost_estimate=pl.CostEstimate(flops=1 << 30, bytes_accessed=8 << 20, transcendentals=0),
        compiler_params=pltpu.CompilerParams(vmem_limit_bytes=16 << 20),
        name="restore",
    )(*parts)


def wave_table(length):
    half = length // 2
    freq = np.concatenate([np.arange(half + 1), np.arange(1, half)])
    angle = 2.0 * np.pi / length * (np.arange(length)[:, None] * freq[None, :] % length)
    table = np.where(np.arange(length)[None, :] <= half, np.cos(angle), np.sin(angle))
    doubled = np.where((freq == 0) | (freq == half), 1.0, 2.0) / length
    return table.astype(np.float32), doubled.astype(np.float32)


def window_matrix(gain, table, doubled):
    length = gain.shape[0]
    half = length // 2
    weight = jnp.concatenate([gain[: half + 1], gain[1:half]]) * doubled
    return lax.dot_general(
        table * weight[None, :], table, (((1,), (1,)), ((), ())), precision=lax.Precision.HIGHEST
    )


def on_device(groups, log_crit, col_bins, rate_table, tile_mask, tile_route, filt_x, filt_y):
    span_x, span_y = lax.axis_size("gx"), lax.axis_size("gy")
    devices = span_x * span_y
    size_x, size_y, size_z = log_crit.shape
    blocks_x, blocks_y, blocks_z = tile_mask.shape
    edge = size_x // blocks_x
    tile_count = blocks_x * blocks_y * blocks_z
    bins = col_bins.transpose(1, 2, 0)
    rates = rate_table.T
    cells, sums = [], []
    for first, runs in groups:
        part, total = evaluate(log_crit, bins, rates, tile_mask, first, runs, devices)
        cells.append(part)
        sums.append(total)
    tables = {length: wave_table(length) for length in (filt_x.shape[0], filt_y.shape[0])}
    tables = {length: tuple(jnp.asarray(item) for item in pair) for length, pair in tables.items()}
    matrix_x = window_matrix(filt_x, *tables[filt_x.shape[0]])
    matrix_y = window_matrix(filt_y, *tables[filt_y.shape[0]])
    exchange = functools.partial(
        lax.all_to_all, axis_name=("gx", "gy"), split_axis=0, concat_axis=0, tiled=True
    )
    tile_sums = jnp.concatenate(sums, axis=1).sum(axis=2)
    tile_means = tile_sums.reshape(blocks_y, blocks_z, blocks_x, edge).sum(axis=3) / (edge * edge * edge)
    route = tile_route.transpose(1, 2, 0)
    workers = jnp.arange(span_y, dtype=jnp.int32)
    shares = jnp.where(route[..., None] == workers, tile_means[..., None], 0.0)
    contribution = shares.sum(axis=(0, 1, 2)) / (tile_count // 2)
    pencils = [exchange(part) for part in cells]
    recomb = restore(cells, edge)
    shares_of = [pencils] if len(pencils) < 3 else [pencils[:2], pencils[2:]]
    filtered = [apply_window(parts, matrix_x, matrix_y, span_x, span_y) for parts in shares_of]
    filtered[-1], recomb = lax.optimization_barrier((filtered[-1], recomb))
    filtered[-1], contribution = lax.optimization_barrier((filtered[-1], contribution))
    returned = [exchange(part) for part in filtered]
    mine = workers == lax.axis_index("gy")
    load = jnp.sum(jnp.where(mine, lax.psum(contribution, "gy"), 0.0)).reshape(1, 1)
    smoothed = restore(returned, edge)
    return recomb, smoothed, load


def split_runs(size_z, edge, devices):
    runs = size_z // edge
    smallest = max(1, devices // edge)
    if smallest * 4 != runs:
        return ((0, runs),)
    return ((0, smallest), (smallest, 2 * smallest), (3 * smallest, smallest))


def solution(mesh):
    placed = (
        P("gx", "gy", None),
        P("gx", "gy", None),
        P(),
        P("gx", "gy", None),
        P("gx", "gy", None),
        P(),
        P(),
    )
    devices = mesh.shape["gx"] * mesh.shape["gy"]

    def whole(*args):
        size_z = args[0].shape[2]
        edge = args[0].shape[0] // args[3].shape[0]
        groups = split_runs(size_z, edge, devices)
        return jax.shard_map(
            functools.partial(on_device, groups),
            mesh=mesh,
            in_specs=placed,
            out_specs=(P("gx", "gy", None), P("gx", "gy", None), P("gx", "gy")),
            check_vma=False,
        )(*args)

    return whole
```

```python
import functools

import jax
import jax.numpy as jnp
import numpy as np
from jax import lax
from jax.experimental import pallas as pl
from jax.experimental.pallas import tpu as pltpu
from jax.sharding import PartitionSpec as P

STEEPNESS = 3.0
ROWS = 16
UNROLL = 4


def node_grid(nodes):
    return np.float32(-2.5) + np.float32(5.0) * np.arange(nodes, dtype=np.float32) / np.float32(nodes - 1)


def evaluate_kernel(run_first, runs, edge, devices, mask_ref, field_ref, bins_ref, rate_ref, cells_ref, sums_ref, row_scratch):
    step = pl.program_id(0)
    size_x, rows, size_z = field_ref.shape
    nodes, levels = rate_ref.shape
    planes = cells_ref.shape[1]
    half_nodes = np.float32(0.5 * STEEPNESS) * node_grid(nodes)
    tile_b = step * rows // edge
    tiles_x = size_x // edge
    lane = lax.broadcasted_iota(jnp.int32, (1, size_x), 1)
    level = lax.broadcasted_iota(jnp.int32, (levels, size_x), 0)
    field = field_ref.reshape(size_x * rows, size_z)
    cells = cells_ref.reshape(devices * planes * rows, size_x)

    @pl.when(step % (edge // rows) == 0)
    def _():
        sums_ref[...] = jnp.zeros_like(sums_ref)

    for run in range(runs):
        active = jnp.zeros((1, size_x), jnp.float32)
        for a in range(tiles_x):
            flag = mask_ref[a, tile_b, run_first + run]
            here = (lane >= a * edge) & (lane < (a + 1) * edge)
            active = jnp.where(here & (flag == 1), 0.5, active)
        for y in range(rows):
            onehot = (level == bins_ref[y, pl.ds(run_first + run, 1), :]).astype(jnp.bfloat16)
            row_scratch[run, y] = jnp.dot(rate_ref[...], onehot, preferred_element_type=jnp.float32) * active

    first_z = run_first * edge
    last_z = first_z + runs * edge

    def some_rows(pair, carry):
        for y in [pair * UNROLL + k for k in range(UNROLL)]:
            if first_z == 0:
                turned = field[pl.ds(y, size_x, stride=rows), :][:, :last_z].T
            else:
                turned = field[pl.ds(y, size_x, stride=rows), :].T[first_z:last_z]
            scaled = turned * (0.5 * STEEPNESS)
            for run in range(runs):
                values = scaled[run * edge : (run + 1) * edge]
                total = jnp.broadcast_to(jnp.sum(row_scratch[run, y], axis=0, keepdims=True), values.shape)
                for q in range(nodes):
                    rate = row_scratch[run, y, pl.ds(q, 1), :]
                    total = total + rate * jnp.tanh(values - half_nodes[q])
                plane, first = divmod(run * edge, devices)
                cells[pl.ds(first * planes * rows + plane * rows + y, edge, stride=planes * rows), :] = total
                part = total[0:8]
                for k in range(8, edge, 8):
                    part = part + total[k : k + 8]
                sums_ref[0, run] += part
        return carry

    lax.fori_loop(0, rows // UNROLL, some_rows, 0)


def evaluate(log_crit, bins, rates, tile_mask, run_first, runs, devices):
    size_x, size_y, size_z = log_crit.shape
    edge = size_x // tile_mask.shape[0]
    planes = runs * edge // devices
    tiles_y = tile_mask.shape[1]
    nodes, levels = rates.shape
    steps = size_y // ROWS
    return pl.pallas_call(
        functools.partial(evaluate_kernel, run_first, runs, edge, devices),
        grid=(steps,),
        in_specs=[
            pl.BlockSpec(memory_space=pltpu.SMEM),
            pl.BlockSpec((size_x, ROWS, size_z), lambda j: (0, j, 0)),
            pl.BlockSpec((ROWS, bins.shape[1], size_x), lambda j: (j, 0, 0)),
            pl.BlockSpec((nodes, levels), lambda j: (0, 0)),
        ],
        out_specs=[
            pl.BlockSpec((devices, planes, ROWS, size_x), lambda j: (0, 0, j, 0)),
            pl.BlockSpec((1, runs, 8, size_x), lambda j: (j * ROWS // edge, 0, 0, 0)),
        ],
        out_shape=[
            jax.ShapeDtypeStruct((devices, planes, size_y, size_x), jnp.float32),
            jax.ShapeDtypeStruct((tiles_y, runs, 8, size_x), jnp.float32),
        ],
        scratch_shapes=[
            pltpu.VMEM((runs, ROWS, nodes, size_x), jnp.float32),
        ],
        cost_estimate=pl.CostEstimate(
            flops=runs * edge * size_x * size_y * nodes * 4, bytes_accessed=6 << 20, transcendentals=0
        ),
        name="evaluate",
    )(tile_mask, log_crit, bins, rates)


def split(value):
    high = value.astype(jnp.bfloat16)
    low = (value - high.astype(jnp.float32)).astype(jnp.bfloat16)
    return high, low


def product(left, right):
    dot = functools.partial(jnp.dot, preferred_element_type=jnp.float32)
    return dot(left[0], right[0]) + (dot(left[0], right[1]) + dot(left[1], right[0]))


def window_kernel(span_x, span_y, first_planes, x_ref, y_ref, *refs):
    plane_refs, out_ref = refs[:-1], refs[-1]
    rows, lanes = out_ref.shape[-2:]
    step = pl.program_id(0)

    def assemble(ref):
        return jnp.concatenate(
            [
                jnp.concatenate([ref[i * span_y + j, 0] for i in range(span_x)], axis=1)
                for j in range(span_y)
            ],
            axis=0,
        )

    plane = assemble(plane_refs[0])
    if len(plane_refs) == 2:
        plane = jnp.where(step < first_planes, plane, assemble(plane_refs[1]))
    along_y = product(split(y_ref[...]), split(plane))
    both = product(split(along_y), split(x_ref[...]))
    for i in range(span_x):
        for j in range(span_y):
            out_ref[i * span_y + j, 0] = both[j * rows : (j + 1) * rows, i * lanes : (i + 1) * lanes]


def apply_window(parts, matrix_x, matrix_y, span_x, span_y):
    devices, first_planes, rows, lanes = parts[0].shape
    count = sum(part.shape[1] for part in parts)
    size_x, size_y = matrix_x.shape[0], matrix_y.shape[0]
    block = (devices, 1, rows, lanes)
    specs = [pl.BlockSpec(block, lambda p: (0, jnp.minimum(p, first_planes - 1), 0, 0))]
    if len(parts) == 2:
        specs.append(pl.BlockSpec(block, lambda p: (0, jnp.maximum(p - first_planes, 0), 0, 0)))
    return pl.pallas_call(
        functools.partial(window_kernel, span_x, span_y, first_planes),
        grid=(count,),
        in_specs=[
            pl.BlockSpec((size_x, size_x), lambda p: (0, 0)),
            pl.BlockSpec((size_y, size_y), lambda p: (0, 0)),
            *specs,
        ],
        out_specs=pl.BlockSpec(block, lambda p: (0, p, 0, 0)),
        out_shape=jax.ShapeDtypeStruct((devices, count, rows, lanes), jnp.float32),
        cost_estimate=pl.CostEstimate(
            flops=count * 6 * size_x * size_y * (size_x + size_y), bytes_accessed=4 << 20, transcendentals=0
        ),
        name="window",
    )(matrix_x, matrix_y, *parts)


def restore_kernel(edge, count, *refs):
    parts, out_ref = refs[:count], refs[count]
    size_x, rows, size_z = out_ref.shape
    out = out_ref.reshape(size_x * rows, size_z)

    for y in range(rows):
        pieces = []
        for part in parts:
            devices, planes = part.shape[:2]
            flat = part.reshape(devices * planes * rows, size_x)
            for plane in range(planes):
                pieces.append(flat[pl.ds(plane * rows + y, devices, stride=planes * rows), :])
        whole = pieces[0] if len(pieces) == 1 else jnp.concatenate(pieces, axis=0)
        out[pl.ds(y, size_x, stride=rows), :] = whole.T


def restore(parts, edge):
    size_y, size_x = parts[0].shape[2:]
    size_z = sum(part.shape[0] * part.shape[1] for part in parts)
    return pl.pallas_call(
        functools.partial(restore_kernel, edge, len(parts)),
        grid=(size_y // ROWS,),
        in_specs=[
            pl.BlockSpec((*part.shape[:2], ROWS, size_x), lambda j: (0, 0, j, 0)) for part in parts
        ],
        out_specs=pl.BlockSpec((size_x, ROWS, size_z), lambda j: (0, j, 0)),
        out_shape=jax.ShapeDtypeStruct((size_x, size_y, size_z), jnp.float32),
        cost_estimate=pl.CostEstimate(flops=1 << 30, bytes_accessed=8 << 20, transcendentals=0),
        compiler_params=pltpu.CompilerParams(vmem_limit_bytes=54_000_000),
        name="restore",
    )(*parts)


def wave_table(length):
    half = length // 2
    freq = np.concatenate([np.arange(half + 1), np.arange(1, half)])
    angle = 2.0 * np.pi / length * (np.arange(length)[:, None] * freq[None, :] % length)
    table = np.where(np.arange(length)[None, :] <= half, np.cos(angle), np.sin(angle))
    doubled = np.where((freq == 0) | (freq == half), 1.0, 2.0) / length
    return table.astype(np.float32), doubled.astype(np.float32)


def window_matrix(gain, table, doubled):
    length = gain.shape[0]
    half = length // 2
    weight = jnp.concatenate([gain[: half + 1], gain[1:half]]) * doubled
    return lax.dot_general(
        table * weight[None, :], table, (((1,), (1,)), ((), ())), precision=lax.Precision.HIGHEST
    )


def on_device(groups, log_crit, col_bins, rate_table, tile_mask, tile_route, filt_x, filt_y):
    span_x, span_y = lax.axis_size("gx"), lax.axis_size("gy")
    devices = span_x * span_y
    size_x, size_y, size_z = log_crit.shape
    blocks_x, blocks_y, blocks_z = tile_mask.shape
    edge = size_x // blocks_x
    tile_count = blocks_x * blocks_y * blocks_z
    bins = col_bins.transpose(1, 2, 0)
    rates = rate_table.T
    cells, sums = [], []
    for first, runs in groups:
        part, total = evaluate(log_crit, bins, rates, tile_mask, first, runs, devices)
        cells.append(part)
        sums.append(total)
    tables = {length: wave_table(length) for length in (filt_x.shape[0], filt_y.shape[0])}
    tables = {length: tuple(jnp.asarray(item) for item in pair) for length, pair in tables.items()}
    matrix_x = window_matrix(filt_x, *tables[filt_x.shape[0]])
    matrix_y = window_matrix(filt_y, *tables[filt_y.shape[0]])
    exchange = functools.partial(
        lax.all_to_all, axis_name=("gx", "gy"), split_axis=0, concat_axis=0, tiled=True
    )
    tile_sums = jnp.concatenate(sums, axis=1).sum(axis=2)
    tile_means = tile_sums.reshape(blocks_y, blocks_z, blocks_x, edge).sum(axis=3) / (edge * edge * edge)
    route = tile_route.transpose(1, 2, 0)
    workers = jnp.arange(span_y, dtype=jnp.int32)
    shares = jnp.where(route[..., None] == workers, tile_means[..., None], 0.0)
    contribution = shares.sum(axis=(0, 1, 2)) / (tile_count // 2)
    pencils = [exchange(part) for part in cells]
    recomb = restore(cells, edge)
    shares_of = [pencils] if len(pencils) < 3 else [pencils[:2], pencils[2:]]
    filtered = [apply_window(parts, matrix_x, matrix_y, span_x, span_y) for parts in shares_of]
    filtered[-1], recomb = lax.optimization_barrier((filtered[-1], recomb))
    filtered[-1], contribution = lax.optimization_barrier((filtered[-1], contribution))
    returned = [exchange(part) for part in filtered]
    mine = workers == lax.axis_index("gy")
    load = jnp.sum(jnp.where(mine, lax.psum(contribution, "gy"), 0.0)).reshape(1, 1)
    smoothed = restore(returned, edge)
    return recomb, smoothed, load


def split_runs(size_z, edge, devices):
    runs = size_z // edge
    smallest = max(1, devices // edge)
    if smallest * 4 != runs:
        return ((0, runs),)
    return ((0, smallest), (smallest, 2 * smallest), (3 * smallest, smallest))


def solution(mesh):
    placed = (
        P("gx", "gy", None),
        P("gx", "gy", None),
        P(),
        P("gx", "gy", None),
        P("gx", "gy", None),
        P(),
        P(),
    )
    devices = mesh.shape["gx"] * mesh.shape["gy"]

    def whole(*args):
        size_z = args[0].shape[2]
        edge = args[0].shape[0] // args[3].shape[0]
        groups = split_runs(size_z, edge, devices)
        return jax.shard_map(
            functools.partial(on_device, groups),
            mesh=mesh,
            in_specs=placed,
            out_specs=(P("gx", "gy", None), P("gx", "gy", None), P("gx", "gy")),
            check_vma=False,
        )(*args)

    return whole
```
